32 devices in a mesh: band: 8 (over y, x, core), chan: 4 (over z).
Axes of the slice: x: 2, y: 2, z: 4, core: 2. Of those that a mesh axis runs over, the one named last changes fastest.
Arguments:
- grid_feat: bfloat16 [2048, 468], P('band'), may hold values from -6 to 6
- w_embed: bfloat16 [468, 384], replicated, may hold values from -0.25 to 0.25
- w_send: bfloat16 [384, 384], P(None, 'chan'), may hold values from -0.3125 to 0.3125
- w_recv: bfloat16 [384, 384], P(None, 'chan'), may hold values from -0.3125 to 0.3125
- mesh_nodes: bfloat16 [2048, 384], P('band'), may hold values from -6 to 6
- mesh_cot: bfloat16 [2048, 384], P('band', 'chan'), may hold values from -0.049804688 to 0.049804688
- send_index: int32 [8, 2, 64], P('band'), may hold values from -1 to 255, as said below
- edge_source: int32 [32768], P('band'), may hold values from 0 to 383, as said below
- edge_receiver: int32 [32768], P('band'), may hold values from 0 to 255
Outputs:
- mesh_out: bfloat16 [2048, 384], P('band', 'chan')
- grad_embed: float32 [468, 384], P(None, 'chan')
- grad_send: float32 [384, 384], P(None, 'chan')
- grad_recv: float32 [384, 384], P(None, 'chan')
The draws below stay inside these ranges and needn't reach their ends.
Inputs may be any that keep to these rules, and one draw needn't show every extreme that they name: `send_index`: A block's first c slots hold rows (c from 32 to 64) and the rest hold -1; block [0, 0] and block [8 - 1, 1] hold only -1; for every band s one of its two blocks that are not all -1 has all 64 slots used (block [0, 1] for band 0, block [8 - 1, 0] for band 8 - 1). `edge_source`: every edge names a used slot of its partition, and every used slot is named by some edge of its partition.
All inputs are finite; a program needn't handle non-finite values.
Results may differ from the reference program's by a relative error of at most 0.011.
Values may be sent and summed in bfloat16 or wider, within the bound.
A program may use at most 64 MiB of HBM per device.

```python
import jax
import jax.numpy as jnp
from jax import lax

F = 468
L = 384
H = 384
G_DEV = 256
E_DEV = 4096
M_DEV = 256
CAP = 64
GRID = 2048
EDGES = 32768
MESH = 2048
N_BAND = 8


def count_table(key):
    lowest = max(2, CAP // 2)
    counts = jax.random.randint(jax.random.fold_in(key, 11), (N_BAND, 2), lowest, CAP + 1)
    full_side = jax.random.randint(jax.random.fold_in(key, 12), (N_BAND,), 0, 2)
    band = jnp.arange(N_BAND, dtype=jnp.int32)
    full_side = jnp.where(band == 0, 1, jnp.where(band == N_BAND - 1, 0, full_side))
    side = jnp.arange(2, dtype=jnp.int32)[None, :]
    counts = jnp.where(side == full_side[:, None], CAP, counts)
    exists = (side == 1) & (band[:, None] < N_BAND - 1) | (side == 0) & (band[:, None] > 0)
    return jnp.where(exists, counts, 0).astype(jnp.int32)


def draw_send_index(key, part):
    counts = count_table(key)
    grid_rows = jax.random.randint(jax.random.fold_in(key, 13), (N_BAND, 2, CAP), 0, G_DEV)
    slot_pos = jnp.arange(CAP, dtype=jnp.int32)[None, None, :]
    return jnp.where(slot_pos < counts[:, :, None], grid_rows, -1).astype(jnp.int32)


def draw_edge_source(key, part):
    counts = count_table(key)
    nothing = jnp.zeros((1,), dtype=jnp.int32)
    below = jnp.concatenate([nothing, counts[:-1, 1]])[:, None]
    above = jnp.concatenate([counts[1:, 0], nothing])[:, None]
    slot_width = G_DEV + 2 * CAP
    position = jnp.arange(E_DEV, dtype=jnp.int32)[None, :]
    valid_total = G_DEV + below + above
    drawn = jax.random.randint(jax.random.fold_in(key, 14), (N_BAND, E_DEV), 0, valid_total)
    placed = jnp.where(drawn < G_DEV + below, drawn, drawn - below + CAP)
    valid = (position < G_DEV) | (position >= G_DEV) & (position < G_DEV + below) | (position >= G_DEV + CAP) & (position < G_DEV + CAP + above)
    leading = jnp.where(valid, position, position % G_DEV)
    ordered = jnp.where(position < slot_width, leading, placed).astype(jnp.int32)
    row_keys = jax.random.split(jax.random.fold_in(key, 16), N_BAND)
    orders = jax.vmap(lambda one_key: jax.random.permutation(one_key, E_DEV))(row_keys)
    shuffled = jnp.take_along_axis(ordered, orders.astype(jnp.int32), axis=1)
    return shuffled.reshape(-1).astype(jnp.int32)


def place_ends(result, rng, smallest, high):
    index_at = [jax.random.randint(jax.random.fold_in(rng, axis), (), 0, length) for axis, length in enumerate(result.shape)]
    longest = result.shape.index(max(result.shape))
    neighbour = index_at[:longest] + [(index_at[longest] + 1) % result.shape[longest]] + index_at[longest + 1:]
    return result.at[tuple(index_at)].set(smallest).at[tuple(neighbour)].set(high)


def shard_levels(stream_key, shape, pieces, smallest, largest):
    def one(axis_at, shards_of):
        draws = jax.random.uniform(jax.random.fold_in(jax.random.fold_in(stream_key, 6), axis_at), (shards_of,), jnp.float32, smallest / len(pieces), largest / len(pieces))
        return jnp.repeat(jnp.exp(draws), shape[axis_at] // shards_of).reshape((-1,) + (1,) * (len(shape) - axis_at - 1))

    factor_of = one(*pieces[0])
    for cut in pieces[1:]:
        factor_of = factor_of * one(*cut)
    return factor_of


def scatter_about(stream_key, extent, spread, most, shards=(), held_as=jnp.bfloat16):
    result = spread * jax.random.normal(stream_key, extent, jnp.float32)
    if shards:
        result = result * shard_levels(stream_key, extent, shards, -0.22, 0.18)
    return jnp.clip(result, -most, most).astype(held_as)


def setup_inputs(seed: int = 0) -> dict:
    seeds = jax.random.split(jax.random.key(seed), 10)
    return {
        "grid_feat": scatter_about(seeds[0], (GRID, F), 1.0, 6.0, ((0, 8),)),
        "w_embed": scatter_about(seeds[1], (F, L), F ** -0.5, 0.25),
        "w_send": scatter_about(seeds[2], (L, H), L ** -0.5, 0.3125, ((1, 4),)),
        "w_recv": scatter_about(seeds[3], (L, H), L ** -0.5, 0.3125, ((1, 4),)),
        "mesh_nodes": scatter_about(seeds[4], (MESH, L), 1.0, 6.0, ((0, 8),)),
        "mesh_cot": scatter_about(seeds[5], (MESH, H), 0.008, 0.049804688, ((0, 8), (1, 4))),
        "send_index": draw_send_index(jax.random.fold_in(seeds[9], 71), 0),
        "edge_source": draw_edge_source(jax.random.fold_in(seeds[9], 71), 0),
        "edge_receiver": place_ends(jax.random.randint(seeds[8], (EDGES,), 0, M_DEV), jax.random.fold_in(seeds[8], 1), 0, M_DEV - 1).astype(jnp.int32),
    }


def silu_slope(inputs):
    sigmoid_v = jax.nn.sigmoid(inputs)
    return sigmoid_v * (1.0 + inputs * (1.0 - sigmoid_v))


def reference(grid_feat, w_embed, w_send, w_recv, mesh_nodes, mesh_cot, send_index, edge_source, edge_receiver):
    grid_pre = jnp.dot(grid_feat, w_embed, preferred_element_type=jnp.float32)
    latent = jax.nn.silu(grid_pre).astype(jnp.bfloat16)
    slot_width = G_DEV + 2 * CAP
    blank = jnp.full((1, 2, CAP), -1, dtype=jnp.int32)
    padded_index = jnp.concatenate([blank, send_index.astype(jnp.int32), blank], axis=0)
    below = padded_index[0:N_BAND, 1]
    above = padded_index[2:N_BAND + 2, 0]
    bands = jnp.arange(N_BAND, dtype=jnp.int32)[:, None]
    own_ids = bands * G_DEV + jnp.arange(G_DEV, dtype=jnp.int32)[None, :]
    below_ids = jnp.where(below >= 0, (bands - 1) * G_DEV + below, GRID)
    above_ids = jnp.where(above >= 0, (bands + 1) * G_DEV + above, GRID)
    slot_node = jnp.concatenate([own_ids, below_ids, above_ids], axis=1).astype(jnp.int32)

    def partition(items):
        node_ids, sources, receivers, nodes, cotan = items
        rows = latent[jnp.minimum(node_ids, GRID - 1)]
        send_proj = jnp.dot(rows, w_send, preferred_element_type=jnp.float32)
        recv_proj = jnp.dot(nodes, w_recv, preferred_element_type=jnp.float32)
        edge_pre = send_proj[sources] + recv_proj[receivers]
        message = jax.nn.silu(edge_pre).astype(jnp.bfloat16)
        out_block = jax.ops.segment_sum(message.astype(jnp.float32), receivers, M_DEV).astype(jnp.bfloat16)
        edge_grad = (cotan[receivers].astype(jnp.float32) * silu_slope(edge_pre)).astype(jnp.bfloat16)
        slot_grad = jax.ops.segment_sum(edge_grad.astype(jnp.float32), sources, slot_width).astype(jnp.bfloat16)
        recv_grad = jax.ops.segment_sum(edge_grad.astype(jnp.float32), receivers, M_DEV).astype(jnp.bfloat16)
        send_part = jnp.dot(rows.T, slot_grad, preferred_element_type=jnp.float32)
        recv_part = jnp.dot(nodes.T, recv_grad, preferred_element_type=jnp.float32)
        slot_back = jnp.dot(slot_grad, w_send.T, preferred_element_type=jnp.float32)
        return out_block, send_part, recv_part, slot_back

    out_blocks, send_parts, recv_parts, slot_backs = lax.map(partition, (
        slot_node,
        edge_source.reshape(N_BAND, E_DEV).astype(jnp.int32),
        edge_receiver.reshape(N_BAND, E_DEV).astype(jnp.int32),
        mesh_nodes.reshape(N_BAND, M_DEV, L),
        mesh_cot.reshape(N_BAND, M_DEV, H)))
    mesh_out = out_blocks.reshape(MESH, H)
    grad_send = jnp.sum(send_parts, axis=0)
    grad_recv = jnp.sum(recv_parts, axis=0)
    grid_grad = jax.ops.segment_sum(slot_backs.reshape(-1, L), slot_node.reshape(-1), GRID)
    pre_grad = (grid_grad * silu_slope(grid_pre)).astype(jnp.bfloat16)
    grad_embed = jnp.dot(grid_feat.T, pre_grad, preferred_element_type=jnp.float32)
    return mesh_out, grad_embed, grad_send, grad_recv
```

```python
import functools
import math

import jax
import jax.numpy as jnp
from jax import lax
from jax.experimental import pallas as pl
from jax.experimental.pallas import tpu as pltpu
from jax.sharding import PartitionSpec as P

BF = jnp.bfloat16
F32 = jnp.float32
MESH = pl.DeviceIdType.MESH


def mm(a, b):
    return lax.dot_general(a, b, (((1,), (0,)), ((), ())), preferred_element_type=F32)


def mm_nt(a, b):
    return lax.dot_general(a, b, (((1,), (1,)), ((), ())), preferred_element_type=F32)


def eye(size):
    row = lax.broadcasted_iota(jnp.int32, (size, size), 0)
    col = lax.broadcasted_iota(jnp.int32, (size, size), 1)
    return jnp.where(row == col, 1.0, 0.0).astype(BF)


def sigmoid(v):
    return 0.5 + 0.5 * jnp.tanh(0.5 * v)


def flip(index, bit):
    step = 1 << bit
    return index + step - 2 * step * lax.rem(lax.div(index, step), 2)


def body(
    bands, chans, chunk,
    feat, embed, wsend, wrecv, nodes, cot, send, source, receiver,
    mesh_out, early_out, late_out,
    latent, outgoing, outer, tables, acc, slots_out, returned, back_out, back_in,
    xs1, xr1, snd1, rcv1, fin1, xs2, xr2, snd2, rcv2, fin2,
    row_send, row_recv, ret_send, ret_recv, back_send, back_recv, sum_send, sum_recv,
):
    band = lax.axis_index("band")
    chan = lax.axis_index("chan")
    bits = bands.bit_length() - 1
    width = wsend.shape[1]
    grid = feat.shape[0]
    mesh_count = nodes.shape[0]
    cap = outgoing.shape[0] // 2
    slots = grid + 2 * cap
    half = width // 2
    left = lax.rem(band + bands - 1, bands)
    right = lax.rem(band + 1, bands)
    partners = [flip(band, bit) for bit in range(bits)]
    others = [lax.rem(chan + step, chans) for step in range(1, chans)]

    barrier = pltpu.get_barrier_semaphore()
    for peer in [left, right] + partners[1:]:
        pl.semaphore_signal(barrier, inc=1, device_id=(peer, chan), device_id_type=MESH)
    for peer in others:
        pl.semaphore_signal(barrier, inc=1, device_id=(band, peer), device_id_type=MESH)

    def remote(src, dst, send_sem, recv_sem, to_band, to_chan):
        return pltpu.make_async_remote_copy(
            src_ref=src, dst_ref=dst, send_sem=send_sem, recv_sem=recv_sem,
            device_id=(to_band, to_chan), device_id_type=MESH,
        )

    grid_pre = mm(feat[...], embed[...])
    latent[...] = (grid_pre * sigmoid(grid_pre)).astype(BF)
    own = mm(latent[...], wsend[...]).astype(BF)
    picks = lax.broadcasted_iota(jnp.int32, (grid, 2 * cap), 0) == send[...]
    pick_rows = jnp.transpose(jnp.where(picks, 1.0, 0.0)).astype(BF)
    outgoing[...] = mm(pick_rows, own).astype(BF)
    pl.semaphore_wait(barrier, 2 + (bits - 1) + (chans - 1))
    low, high = pl.ds(0, cap), pl.ds(cap, cap)
    rows = [
        remote(outgoing.at[low], outer.at[high], row_send.at[0], row_recv.at[0], left, chan),
        remote(outgoing.at[high], outer.at[low], row_send.at[1], row_recv.at[1], right, chan),
    ]
    for copy in rows:
        copy.start()

    turn = eye(width)
    tables[:width, :grid] = mm_nt(turn, own).astype(BF)
    tables[:width, slots:] = mm_nt(turn, mm(nodes[...], wrecv[...]).astype(BF)).astype(BF)
    tables[width:, :slots] = jnp.zeros((width, slots), BF)
    tables[width:, slots:] = mm_nt(turn, cot[...]).astype(BF)
    acc[...] = jnp.zeros_like(acc)
    choose = lax.broadcasted_iota(jnp.int32, (width, embed.shape[1]), 1) == (
        lax.broadcasted_iota(jnp.int32, (width, embed.shape[1]), 0) + chan * width
    )
    mine = mm_nt(jnp.where(choose, 1.0, 0.0).astype(BF), embed[...]).astype(BF)
    pre_mine = mm_nt(mine, feat[...])
    gate = sigmoid(pre_mine)
    slope_mine = gate * (1.0 + pre_mine * (1.0 - gate))
    for copy in rows:
        copy.wait()
    tables[:width, grid:slots] = mm_nt(turn, outer[...]).astype(BF)

    def edges(step, carry):
        src = source[pl.ds(step, 1), :]
        rec = receiver[pl.ds(step, 1), :]
        hot = jnp.concatenate(
            [
                jnp.where(lax.broadcasted_iota(jnp.int32, (slots, chunk), 0) == src, 1.0, 0.0),
                jnp.where(lax.broadcasted_iota(jnp.int32, (mesh_count, chunk), 0) == rec, 1.0, 0.0),
            ],
            axis=0,
        ).astype(BF)
        drawn = mm(tables[...], hot)
        pre = drawn[:width]
        gate = sigmoid(pre)
        message = pre * gate
        grad = drawn[width:] * (gate + message * (1.0 - gate))
        acc[...] += mm_nt(jnp.concatenate([message, grad], axis=0).astype(BF), hot)
        return carry

    lax.fori_loop(0, source.shape[0], edges, 0)

    slots_out[...] = mm_nt(eye(2 * cap), acc[width:, grid:slots].astype(BF)).astype(BF)
    backs = [
        remote(slots_out.at[low], returned.at[high], ret_send.at[0], ret_recv.at[0], left, chan),
        remote(slots_out.at[high], returned.at[low], ret_send.at[1], ret_recv.at[1], right, chan),
    ]
    for copy in backs:
        copy.start()
    latents = embed.shape[1]
    xs1[:, :latents] = mm(acc[width:, slots:].astype(BF), nodes[...]).astype(BF)
    mesh_out[...] = mm_nt(eye(mesh_count), acc[:width, slots:].astype(BF)).astype(BF)
    for copy in backs:
        copy.wait()
    ret_t = mm_nt(turn, returned[...]).astype(BF)
    total = (acc[width:, :grid].astype(BF).astype(F32) + mm(ret_t, pick_rows)).astype(BF)

    sums = []
    for at, peer in enumerate(others):
        block = wsend[pl.ds(pl.multiple_of(peer * width, width), width), :]
        back_out[at] = mm(block, total).astype(BF)
        copy = remote(back_out.at[at], back_in.at[at], back_send.at[at], back_recv.at[at], band, peer)
        copy.start()
        sums.append(copy)
    grid_grad = mm(wsend[pl.ds(pl.multiple_of(chan * width, width), width), :], total)
    xs1[:, latents:] = mm(total, latent[...]).astype(BF)

    my_half = pl.ds(pl.multiple_of(lax.rem(band, 2) * half, half), half)
    its_half = pl.ds(pl.multiple_of((1 - lax.rem(band, 2)) * half, half), half)

    def reduction(base, xs, xr, snd, rcv, fin):
        middle = xs.shape[1] // 2
        copy = remote(
            xs.at[its_half], xr, sum_send.at[base], sum_recv.at[base], partners[0], chan
        )
        copy.start()
        yield
        copy.wait()
        value = xs[my_half, :].astype(F32) + xr[...].astype(F32)
        for at in range(bits - 1):
            snd[at] = value.astype(BF)
            pair = []
            for side, bit in enumerate((1 + at, bits - 1 - at)):
                cut = pl.ds(side * middle, middle)
                sem = base + 1 + 2 * at + side
                pair.append(
                    remote(
                        snd.at[at, :, cut], rcv.at[at, :, cut],
                        sum_send.at[sem], sum_recv.at[sem], partners[bit], chan,
                    )
                )
            for copy in pair:
                copy.start()
            yield
            for copy in pair:
                copy.wait()
            value = snd[at].astype(F32) + rcv[at].astype(F32)
        fin[my_half, :] = value
        sem = base + 1 + 2 * (bits - 1)
        copy = remote(
            fin.at[my_half], fin.at[my_half], sum_send.at[sem], sum_recv.at[sem], partners[0], chan
        )
        copy.start()
        yield
        copy.wait()
        yield

    early = reduction(0, xs1, xr1, snd1, rcv1, fin1)
    late = reduction(2 * bits, xs2, xr2, snd2, rcv2, fin2)
    next(early)
    next(early)
    for at, copy in enumerate(sums):
        copy.wait()
        grid_grad = grid_grad + back_in[at].astype(F32)
    pre_grad = (grid_grad * slope_mine).astype(BF)
    inputs = feat.shape[1]
    if inputs < xs2.shape[1]:
        xs2[...] = jnp.zeros_like(xs2)
    xs2[:, :inputs] = mm(pre_grad, feat[...]).astype(BF)
    next(late)
    for _ in range(bits - 1):
        next(early)
        next(late)
    next(early)
    early_out[...] = fin1[...]
    next(late)
    next(late)
    late_out[...] = fin2[...]


def on_device(
    grid_feat, w_embed, w_send, w_recv, mesh_nodes, mesh_cot, send_index, edge_source, edge_receiver
):
    bands = lax.axis_size("band")
    chans = lax.axis_size("chan")
    bits = bands.bit_length() - 1
    grid, inputs = grid_feat.shape
    latents, width = w_send.shape
    mesh_count = mesh_nodes.shape[0]
    cap = send_index.shape[2]
    slots = grid + 2 * cap
    half = width // 2
    chunk = math.gcd(edge_source.shape[0], 1024)
    wide1 = 2 * latents
    wide2 = -(-inputs // 256) * 256
    steps = max(bits - 1, 1)
    vmem = pl.BlockSpec(memory_space=pltpu.VMEM)
    mesh_out, early, late = pl.pallas_call(
        functools.partial(body, bands, chans, chunk),
        out_shape=(
            jax.ShapeDtypeStruct((mesh_count, width), BF),
            jax.ShapeDtypeStruct((width, wide1), F32),
            jax.ShapeDtypeStruct((width, wide2), F32),
        ),
        in_specs=[vmem] * 9,
        out_specs=(vmem,) * 3,
        scratch_shapes=[
            pltpu.VMEM((grid, latents), BF),
            pltpu.VMEM((2 * cap, width), BF),
            pltpu.VMEM((2 * cap, width), BF),
            pltpu.VMEM((2 * width, slots + mesh_count), BF),
            pltpu.VMEM((2 * width, slots + mesh_count), F32),
            pltpu.VMEM((2 * cap, width), BF),
            pltpu.VMEM((2 * cap, width), BF),
            pltpu.VMEM((chans - 1, width, grid), BF),
            pltpu.VMEM((chans - 1, width, grid), BF),
        ]
        + [
            pltpu.VMEM(shape, kind)
            for wide in (wide1, wide2)
            for shape, kind in (
                ((width, wide), BF),
                ((half, wide), BF),
                ((steps, half, wide), BF),
                ((steps, half, wide), BF),
                ((width, wide), F32),
            )
        ]
        + [
            pltpu.SemaphoreType.DMA((count,))
            for count in (2, 2, 2, 2, chans - 1, chans - 1, 4 * bits, 4 * bits)
        ],
        compiler_params=pltpu.CompilerParams(collective_id=0, has_side_effects=True),
    )(
        grid_feat, w_embed, w_send, w_recv, mesh_nodes, mesh_cot,
        send_index.reshape(1, 2 * cap),
        edge_source.reshape(-1, chunk),
        edge_receiver.reshape(-1, chunk),
    )
    return (
        mesh_out,
        late[:, :inputs].T,
        early[:, latents:].T,
        early[:, :latents].T,
    )


def solution(mesh):
    placed = (
        P("band", None),
        P(),
        P(None, "chan"),
        P(None, "chan"),
        P("band", None),
        P("band", "chan"),
        P("band", None, None),
        P("band"),
        P("band"),
    )
    return jax.shard_map(
        on_device,
        mesh=mesh,
        in_specs=placed,
        out_specs=(P("band", "chan"), P(None, "chan"), P(None, "chan"), P(None, "chan")),
        check_vma=False,
    )
```

```python
import functools
import math

import jax
import jax.numpy as jnp
from jax import lax
from jax.experimental import pallas as pl
from jax.experimental.pallas import tpu as pltpu
from jax.sharding import PartitionSpec as P

BF = jnp.bfloat16
F32 = jnp.float32
MESH = pl.DeviceIdType.MESH


def mm(a, b):
    return lax.dot_general(a, b, (((1,), (0,)), ((), ())), preferred_element_type=F32)


def mm_tn(a, b):
    return lax.dot_general(a, b, (((0,), (0,)), ((), ())), preferred_element_type=F32)


def mm_nt(a, b):
    return lax.dot_general(a, b, (((1,), (1,)), ((), ())), preferred_element_type=F32)


def eye(size):
    row = lax.broadcasted_iota(jnp.int32, (size, size), 0)
    col = lax.broadcasted_iota(jnp.int32, (size, size), 1)
    return jnp.where(row == col, 1.0, 0.0).astype(BF)


def sigmoid(v):
    return 0.5 + 0.5 * jnp.tanh(0.5 * v)


def flip(index, bit):
    step = 1 << bit
    return index + step - 2 * step * lax.rem(lax.div(index, step), 2)


def body(
    bands, chans, chunk,
    feat, embed, wsend, wrecv, nodes, cot, send, source, receiver,
    mesh_out, late_out, send_out, recv_out,
    latent, back_weight, outgoing, outer, tables, acc, slots_out, returned, back_out, back_in,
    xs1, xr1, snd1, rcv1, fin1, xs2, xr2, snd2, rcv2, fin2,
    row_send, row_recv, ret_send, ret_recv, back_send, back_recv, sum_send, sum_recv,
):
    band = lax.axis_index("band")
    chan = lax.axis_index("chan")
    bits = bands.bit_length() - 1
    width = wsend.shape[0]
    grid = feat.shape[1]
    mesh_count = nodes.shape[0]
    cap = outgoing.shape[0] // 2
    slots = grid + 2 * cap
    half = width // 2
    left = lax.rem(band + bands - 1, bands)
    right = lax.rem(band + 1, bands)
    partners = [flip(band, bit) for bit in range(bits)]
    others = [lax.rem(chan + step, chans) for step in range(1, chans)]

    barrier = pltpu.get_barrier_semaphore()
    for peer in [left, right] + partners[1:]:
        pl.semaphore_signal(barrier, inc=1, device_id=(peer, chan), device_id_type=MESH)
    for peer in others:
        pl.semaphore_signal(barrier, inc=1, device_id=(band, peer), device_id_type=MESH)

    def remote(src, dst, send_sem, recv_sem, to_band, to_chan):
        return pltpu.make_async_remote_copy(
            src_ref=src, dst_ref=dst, send_sem=send_sem, recv_sem=recv_sem,
            device_id=(to_band, to_chan), device_id_type=MESH,
        )

    grid_pre = mm_tn(feat[...], embed[...])
    latent[...] = (grid_pre * sigmoid(grid_pre)).astype(BF)
    own = mm_nt(wsend[...], latent[...]).astype(BF)
    picks = lax.broadcasted_iota(jnp.int32, (grid, 2 * cap), 0) == jnp.concatenate(
        [send[0, 0:1, :], send[0, 1:2, :]], axis=1
    )
    pick_rows = jnp.transpose(jnp.where(picks, 1.0, 0.0)).astype(BF)
    outgoing[...] = mm_nt(pick_rows, own).astype(BF)
    pl.semaphore_wait(barrier, 2 + (bits - 1) + (chans - 1))
    low, high = pl.ds(0, cap), pl.ds(cap, cap)
    rows = [
        remote(outgoing.at[low], outer.at[high], row_send.at[0], row_recv.at[0], left, chan),
        remote(outgoing.at[high], outer.at[low], row_send.at[1], row_recv.at[1], right, chan),
    ]
    for copy in rows:
        copy.start()

    turn = eye(width)
    tables[:width, :grid] = own
    tables[:width, slots:] = mm_nt(wrecv[...], nodes[...]).astype(BF)
    tables[width:, :slots] = jnp.zeros((width, slots), BF)
    tables[width:, slots:] = cot[...]
    acc[...] = jnp.zeros_like(acc)
    back_weight[...] = mm_nt(eye(wsend.shape[1]), wsend[...]).astype(BF)
    choose = lax.broadcasted_iota(jnp.int32, (width, embed.shape[1]), 1) == (
        lax.broadcasted_iota(jnp.int32, (width, embed.shape[1]), 0) + chan * width
    )
    mine = mm_nt(jnp.where(choose, 1.0, 0.0).astype(BF), embed[...]).astype(BF)
    pre_mine = mm(mine, feat[...])
    gate = sigmoid(pre_mine)
    slope_mine = gate * (1.0 + pre_mine * (1.0 - gate))
    for copy in rows:
        copy.wait()
    tables[:width, grid:slots] = mm_nt(turn, outer[...]).astype(BF)

    def edges(step, carry):
        src = source[pl.ds(pl.multiple_of(step * chunk, chunk), chunk)].reshape(1, chunk)
        rec = receiver[pl.ds(pl.multiple_of(step * chunk, chunk), chunk)].reshape(1, chunk)
        hot = jnp.concatenate(
            [
                jnp.where(lax.broadcasted_iota(jnp.int32, (slots, chunk), 0) == src, 1.0, 0.0),
                jnp.where(lax.broadcasted_iota(jnp.int32, (mesh_count, chunk), 0) == rec, 1.0, 0.0),
            ],
            axis=0,
        ).astype(BF)
        drawn = mm(tables[...], hot)
        pre = drawn[:width]
        gate = sigmoid(pre)
        message = pre * gate
        grad = drawn[width:] * (gate + message * (1.0 - gate))
        acc[...] += mm_nt(jnp.concatenate([message, grad], axis=0).astype(BF), hot)
        return carry

    lax.fori_loop(0, source.shape[0] // chunk, edges, 0)

    slots_out[...] = mm_nt(eye(2 * cap), acc[width:, grid:slots].astype(BF)).astype(BF)
    backs = [
        remote(slots_out.at[low], returned.at[high], ret_send.at[0], ret_recv.at[0], left, chan),
        remote(slots_out.at[high], returned.at[low], ret_send.at[1], ret_recv.at[1], right, chan),
    ]
    for copy in backs:
        copy.start()
    latents = embed.shape[1]
    xs1[:, :latents] = mm(acc[width:, slots:].astype(BF), nodes[...]).astype(BF)
    mesh_out[...] = acc[:width, slots:].astype(BF)
    for copy in backs:
        copy.wait()
    ret_t = mm_nt(turn, returned[...]).astype(BF)
    total = (acc[width:, :grid].astype(BF).astype(F32) + mm(ret_t, pick_rows)).astype(BF)

    sums = []
    for at, peer in enumerate(others):
        block = back_weight[pl.ds(pl.multiple_of(peer * width, width), width), :]
        back_out[at] = mm(block, total).astype(BF)
        copy = remote(back_out.at[at], back_in.at[at], back_send.at[at], back_recv.at[at], band, peer)
        copy.start()
        sums.append(copy)
    grid_grad = mm(back_weight[pl.ds(pl.multiple_of(chan * width, width), width), :], total)
    xs1[:, latents:] = mm(total, latent[...]).astype(BF)

    my_half = pl.ds(pl.multiple_of(lax.rem(band, 2) * half, half), half)
    its_half = pl.ds(pl.multiple_of((1 - lax.rem(band, 2)) * half, half), half)

    def reduction(base, xs, xr, snd, rcv, fin):
        middle = xs.shape[1] // 2
        copy = remote(
            xs.at[its_half], xr, sum_send.at[base], sum_recv.at[base], partners[0], chan
        )
        copy.start()
        yield
        copy.wait()
        value = xs[my_half, :].astype(F32) + xr[...].astype(F32)
        for at in range(bits - 1):
            snd[at] = value.astype(BF)
            pair = []
            for side, bit in enumerate((1 + at, bits - 1 - at)):
                cut = pl.ds(side * middle, middle)
                sem = base + 1 + 2 * at + side
                pair.append(
                    remote(
                        snd.at[at, :, cut], rcv.at[at, :, cut],
                        sum_send.at[sem], sum_recv.at[sem], partners[bit], chan,
                    )
                )
            for copy in pair:
                copy.start()
            yield
            for copy in pair:
                copy.wait()
            value = snd[at].astype(F32) + rcv[at].astype(F32)
        fin[my_half, :] = value
        sem = base + 1 + 2 * (bits - 1)
        copy = remote(
            fin.at[my_half], fin.at[my_half], sum_send.at[sem], sum_recv.at[sem], partners[0], chan
        )
        copy.start()
        yield
        copy.wait()
        yield

    early = reduction(0, xs1, xr1, snd1, rcv1, fin1)
    late = reduction(2 * bits, xs2, xr2, snd2, rcv2, fin2)
    next(early)
    next(early)
    for at, copy in enumerate(sums):
        copy.wait()
        grid_grad = grid_grad + back_in[at].astype(F32)
    pre_grad = (grid_grad * slope_mine).astype(BF)
    inputs = feat.shape[0]
    if inputs < xs2.shape[1]:
        xs2[...] = jnp.zeros_like(xs2)
    xs2[:, :inputs] = mm_nt(pre_grad, feat[...]).astype(BF)
    next(late)
    for _ in range(bits - 1):
        next(early)
        next(late)
    next(early)
    recv_out[...] = fin1[:, :latents]
    send_out[...] = fin1[:, latents:]
    next(late)
    next(late)
    late_out[...] = fin2[:, :inputs]


def on_device(
    grid_feat, w_embed, w_send, w_recv, mesh_nodes, mesh_cot, send_index, edge_source, edge_receiver
):
    bands = lax.axis_size("band")
    chans = lax.axis_size("chan")
    bits = bands.bit_length() - 1
    grid, inputs = grid_feat.shape
    latents, width = w_send.shape
    mesh_count = mesh_nodes.shape[0]
    cap = send_index.shape[2]
    slots = grid + 2 * cap
    half = width // 2
    chunk = math.gcd(edge_source.shape[0], 1024)
    wide1 = 2 * latents
    wide2 = -(-inputs // 256) * 256
    steps = max(bits - 1, 1)
    vmem = pl.BlockSpec(memory_space=pltpu.VMEM)
    outs = pl.pallas_call(
        functools.partial(body, bands, chans, chunk),
        out_shape=(
            jax.ShapeDtypeStruct((width, mesh_count), BF),
            jax.ShapeDtypeStruct((width, inputs), F32),
            jax.ShapeDtypeStruct((width, latents), F32),
            jax.ShapeDtypeStruct((width, latents), F32),
        ),
        in_specs=[vmem] * 9,
        out_specs=(vmem,) * 4,
        scratch_shapes=[
            pltpu.VMEM((grid, latents), BF),
            pltpu.VMEM((latents, width), BF),
            pltpu.VMEM((2 * cap, width), BF),
            pltpu.VMEM((2 * cap, width), BF),
            pltpu.VMEM((2 * width, slots + mesh_count), BF),
            pltpu.VMEM((2 * width, slots + mesh_count), F32),
            pltpu.VMEM((2 * cap, width), BF),
            pltpu.VMEM((2 * cap, width), BF),
            pltpu.VMEM((chans - 1, width, grid), BF),
            pltpu.VMEM((chans - 1, width, grid), BF),
        ]
        + [
            pltpu.VMEM(shape, kind)
            for wide in (wide1, wide2)
            for shape, kind in (
                ((width, wide), BF),
                ((half, wide), BF),
                ((steps, half, wide), BF),
                ((steps, half, wide), BF),
                ((width, wide), F32),
            )
        ]
        + [
            pltpu.SemaphoreType.DMA((count,))
            for count in (2, 2, 2, 2, chans - 1, chans - 1, 4 * bits, 4 * bits)
        ],
        compiler_params=pltpu.CompilerParams(collective_id=0, has_side_effects=True),
    )(
        grid_feat.T, w_embed, w_send.T, w_recv.T, mesh_nodes, mesh_cot.T,
        send_index, edge_source, edge_receiver,
    )
    return tuple(out.T for out in outs)


def solution(mesh):
    placed = (
        P("band", None),
        P(),
        P(None, "chan"),
        P(None, "chan"),
        P("band", None),
        P("band", "chan"),
        P("band", None, None),
        P("band"),
        P("band"),
    )
    return jax.shard_map(
        on_device,
        mesh=mesh,
        in_specs=placed,
        out_specs=(P("band", "chan"), P(None, "chan"), P(None, "chan"), P(None, "chan")),
        check_vma=False,
    )
```

```python
import functools
import math

import jax
import jax.numpy as jnp
from jax import lax
from jax.experimental import pallas as pl
from jax.experimental.pallas import tpu as pltpu
from jax.sharding import PartitionSpec as P

BF = jnp.bfloat16
F32 = jnp.float32
MESH = pl.DeviceIdType.MESH


def mm(a, b):
    return lax.dot_general(a, b, (((1,), (0,)), ((), ())), preferred_element_type=F32)


def mm_tn(a, b):
    return lax.dot_general(a, b, (((0,), (0,)), ((), ())), preferred_element_type=F32)


def mm_nt(a, b):
    return lax.dot_general(a, b, (((1,), (1,)), ((), ())), preferred_element_type=F32)


def eye(size):
    row = lax.broadcasted_iota(jnp.int32, (size, size), 0)
    col = lax.broadcasted_iota(jnp.int32, (size, size), 1)
    return jnp.where(row == col, 1.0, 0.0).astype(BF)


def sigmoid(v):
    return 0.5 + 0.5 * jnp.tanh(0.5 * v)


def flip(index, bit):
    step = 1 << bit
    return index + step - 2 * step * lax.rem(lax.div(index, step), 2)


def body(
    bands, chans, chunk,
    feat_in, embed_in, wsend_in, wrecv_in, nodes_in, cot_in, send_in, source_in, receiver_in,
    mesh_out, late_out, send_out, recv_out,
    feat, embed, wsend, wrecv, nodes, cot, send, source, receiver, loads,
    latent, back_weight, outgoing, outer, tables, acc, slots_out, returned, back_out, back_in,
    xs1, xr1, snd1, rcv1, fin1, xs2, xr2, snd2, rcv2, fin2,
    row_send, row_recv, ret_send, ret_recv, back_send, back_recv, sum_send, sum_recv,
):
    band = lax.axis_index("band")
    chan = lax.axis_index("chan")
    bits = bands.bit_length() - 1
    width = wsend.shape[0]
    grid = feat.shape[1]
    mesh_count = nodes.shape[0]
    cap = outgoing.shape[0] // 2
    slots = grid + 2 * cap
    half = width // 2
    left = lax.rem(band + bands - 1, bands)
    right = lax.rem(band + 1, bands)
    partners = [flip(band, bit) for bit in range(bits)]
    others = [lax.rem(chan + step, chans) for step in range(1, chans)]

    barrier = pltpu.get_barrier_semaphore()
    for peer in [left, right] + partners[1:]:
        pl.semaphore_signal(barrier, inc=1, device_id=(peer, chan), device_id_type=MESH)
    for peer in others:
        pl.semaphore_signal(barrier, inc=1, device_id=(band, peer), device_id_type=MESH)

    pulls = {}
    for at, (name, src, dst) in enumerate(
        (
            ("feat", feat_in, feat), ("embed", embed_in, embed), ("send", send_in, send),
            ("wsend", wsend_in, wsend), ("nodes", nodes_in, nodes), ("wrecv", wrecv_in, wrecv),
            ("cot", cot_in, cot), ("source", source_in, source), ("receiver", receiver_in, receiver),
        )
    ):
        pulls[name] = pltpu.make_async_copy(src, dst, loads.at[at])
        pulls[name].start()

    def remote(src, dst, send_sem, recv_sem, to_band, to_chan):
        return pltpu.make_async_remote_copy(
            src_ref=src, dst_ref=dst, send_sem=send_sem, recv_sem=recv_sem,
            device_id=(to_band, to_chan), device_id_type=MESH,
        )

    pulls["send"].wait()
    picks = lax.broadcasted_iota(jnp.int32, (grid, 2 * cap), 0) == jnp.concatenate(
        [send[0, 0:1, :], send[0, 1:2, :]], axis=1
    )
    pick_rows = jnp.transpose(jnp.where(picks, 1.0, 0.0)).astype(BF)
    pulls["feat"].wait()
    pulls["embed"].wait()
    grid_pre = mm_tn(feat[...], embed[...])
    latent[...] = (grid_pre * sigmoid(grid_pre)).astype(BF)
    pulls["wsend"].wait()
    own = mm_nt(wsend[...], latent[...]).astype(BF)
    outgoing[...] = mm_nt(pick_rows, own).astype(BF)
    pl.semaphore_wait(barrier, 2 + (bits - 1) + (chans - 1))
    low, high = pl.ds(0, cap), pl.ds(cap, cap)
    rows = [
        remote(outgoing.at[low], outer.at[high], row_send.at[0], row_recv.at[0], left, chan),
        remote(outgoing.at[high], outer.at[low], row_send.at[1], row_recv.at[1], right, chan),
    ]
    for copy in rows:
        copy.start()

    turn = eye(width)
    for name in ("nodes", "wrecv", "cot", "source", "receiver"):
        pulls[name].wait()
    tables[:width, :grid] = own
    tables[:width, slots:] = mm_nt(wrecv[...], nodes[...]).astype(BF)
    tables[width:, :slots] = jnp.zeros((width, slots), BF)
    tables[width:, slots:] = cot[...]
    acc[...] = jnp.zeros_like(acc)
    back_weight[...] = mm_nt(eye(wsend.shape[1]), wsend[...]).astype(BF)
    choose = lax.broadcasted_iota(jnp.int32, (width, embed.shape[1]), 1) == (
        lax.broadcasted_iota(jnp.int32, (width, embed.shape[1]), 0) + chan * width
    )
    mine = mm_nt(jnp.where(choose, 1.0, 0.0).astype(BF), embed[...]).astype(BF)
    pre_mine = mm(mine, feat[...])
    gate = sigmoid(pre_mine)
    slope_mine = gate * (1.0 + pre_mine * (1.0 - gate))
    for copy in rows:
        copy.wait()
    tables[:width, grid:slots] = mm_nt(turn, outer[...]).astype(BF)

    def edges(step, carry):
        src = source[pl.ds(pl.multiple_of(step * chunk, chunk), chunk)].reshape(1, chunk)
        rec = receiver[pl.ds(pl.multiple_of(step * chunk, chunk), chunk)].reshape(1, chunk)
        hot = jnp.concatenate(
            [
                jnp.where(lax.broadcasted_iota(jnp.int32, (slots, chunk), 0) == src, 1.0, 0.0),
                jnp.where(lax.broadcasted_iota(jnp.int32, (mesh_count, chunk), 0) == rec, 1.0, 0.0),
            ],
            axis=0,
        ).astype(BF)
        drawn = mm(tables[...], hot)
        pre = drawn[:width]
        gate = sigmoid(pre)
        message = pre * gate
        grad = drawn[width:] * (gate + message * (1.0 - gate))
        acc[...] += mm_nt(jnp.concatenate([message, grad], axis=0).astype(BF), hot)
        return carry

    lax.fori_loop(0, source.shape[0] // chunk, edges, 0)

    slots_out[...] = mm_nt(eye(2 * cap), acc[width:, grid:slots].astype(BF)).astype(BF)
    backs = [
        remote(slots_out.at[low], returned.at[high], ret_send.at[0], ret_recv.at[0], left, chan),
        remote(slots_out.at[high], returned.at[low], ret_send.at[1], ret_recv.at[1], right, chan),
    ]
    for copy in backs:
        copy.start()
    latents = embed.shape[1]
    xs1[:, :latents] = mm(acc[width:, slots:].astype(BF), nodes[...]).astype(BF)
    mesh_out[...] = acc[:width, slots:].astype(BF)
    for copy in backs:
        copy.wait()
    ret_t = mm_nt(turn, returned[...]).astype(BF)
    total = (acc[width:, :grid].astype(BF).astype(F32) + mm(ret_t, pick_rows)).astype(BF)

    sums = []
    for at, peer in enumerate(others):
        block = back_weight[pl.ds(pl.multiple_of(peer * width, width), width), :]
        back_out[at] = mm(block, total).astype(BF)
        copy = remote(back_out.at[at], back_in.at[at], back_send.at[at], back_recv.at[at], band, peer)
        copy.start()
        sums.append(copy)
    grid_grad = mm(back_weight[pl.ds(pl.multiple_of(chan * width, width), width), :], total)
    xs1[:, latents:] = mm(total, latent[...]).astype(BF)

    my_half = pl.ds(pl.multiple_of(lax.rem(band, 2) * half, half), half)
    its_half = pl.ds(pl.multiple_of((1 - lax.rem(band, 2)) * half, half), half)

    def reduction(base, xs, xr, snd, rcv, fin):
        middle = xs.shape[1] // 2
        copy = remote(
            xs.at[its_half], xr, sum_send.at[base], sum_recv.at[base], partners[0], chan
        )
        copy.start()
        yield
        copy.wait()
        value = xs[my_half, :].astype(F32) + xr[...].astype(F32)
        for at in range(bits - 1):
            snd[at] = value.astype(BF)
            pair = []
            for side, bit in enumerate((1 + at, bits - 1 - at)):
                cut = pl.ds(side * middle, middle)
                sem = base + 1 + 2 * at + side
                pair.append(
                    remote(
                        snd.at[at, :, cut], rcv.at[at, :, cut],
                        sum_send.at[sem], sum_recv.at[sem], partners[bit], chan,
                    )
                )
            for copy in pair:
                copy.start()
            yield
            for copy in pair:
                copy.wait()
            value = snd[at].astype(F32) + rcv[at].astype(F32)
        fin[my_half, :] = value
        sem = base + 1 + 2 * (bits - 1)
        copy = remote(
            fin.at[my_half], fin.at[my_half], sum_send.at[sem], sum_recv.at[sem], partners[0], chan
        )
        copy.start()
        yield
        copy.wait()
        yield

    early = reduction(0, xs1, xr1, snd1, rcv1, fin1)
    late = reduction(2 * bits, xs2, xr2, snd2, rcv2, fin2)
    for _ in range(bits):
        next(early)
    for at, copy in enumerate(sums):
        copy.wait()
        grid_grad = grid_grad + back_in[at].astype(F32)
    pre_grad = (grid_grad * slope_mine).astype(BF)
    inputs = feat.shape[0]
    if inputs < xs2.shape[1]:
        xs2[...] = jnp.zeros_like(xs2)
    xs2[:, :inputs] = mm_nt(pre_grad, feat[...]).astype(BF)
    next(late)
    next(early)
    next(late)
    next(early)
    recv_out[...] = fin1[:, :latents]
    send_out[...] = fin1[:, latents:]
    for _ in range(bits):
        next(late)
    late_out[...] = fin2[:, :inputs]


def place(count, *refs):
    sems = refs[2 * count]
    copies = [
        pltpu.make_async_copy(refs[at], refs[count + at], sems.at[at]) for at in range(count)
    ]
    for copy in copies:
        copy.start()
    for copy in copies:
        copy.wait()


def on_device(
    grid_feat, w_embed, w_send, w_recv, mesh_nodes, mesh_cot, send_index, edge_source, edge_receiver
):
    bands = lax.axis_size("band")
    chans = lax.axis_size("chan")
    bits = bands.bit_length() - 1
    grid, inputs = grid_feat.shape
    latents, width = w_send.shape
    mesh_count = mesh_nodes.shape[0]
    cap = send_index.shape[2]
    slots = grid + 2 * cap
    half = width // 2
    chunk = math.gcd(edge_source.shape[0], 1024)
    wide1 = 2 * latents
    wide2 = -(-inputs // 256) * 256
    steps = max(bits - 1, 1)
    vmem = pl.BlockSpec(memory_space=pltpu.VMEM)
    arrays = (
        grid_feat.T, w_embed, w_send.T, w_recv.T, mesh_nodes, mesh_cot.T,
        send_index, edge_source, edge_receiver,
    )
    outs = pl.pallas_call(
        functools.partial(body, bands, chans, chunk),
        out_shape=(
            pltpu.VMEM((width, mesh_count), BF),
            pltpu.VMEM((width, inputs), F32),
            pltpu.VMEM((width, latents), F32),
            pltpu.VMEM((width, latents), F32),
        ),
        in_specs=[pl.BlockSpec(memory_space=pl.ANY)] * 9,
        out_specs=(vmem,) * 4,
        scratch_shapes=[
            pltpu.VMEM(array.shape, array.dtype) for array in arrays
        ]
        + [
            pltpu.SemaphoreType.DMA((9,)),
            pltpu.VMEM((grid, latents), BF),
            pltpu.VMEM((latents, width), BF),
            pltpu.VMEM((2 * cap, width), BF),
            pltpu.VMEM((2 * cap, width), BF),
            pltpu.VMEM((2 * width, slots + mesh_count), BF),
            pltpu.VMEM((2 * width, slots + mesh_count), F32),
            pltpu.VMEM((2 * cap, width), BF),
            pltpu.VMEM((2 * cap, width), BF),
            pltpu.VMEM((chans - 1, width, grid), BF),
            pltpu.VMEM((chans - 1, width, grid), BF),
        ]
        + [
            pltpu.VMEM(shape, kind)
            for wide in (wide1, wide2)
            for shape, kind in (
                ((width, wide), BF),
                ((half, wide), BF),
                ((steps, half, wide), BF),
                ((steps, half, wide), BF),
                ((width, wide), F32),
            )
        ]
        + [
            pltpu.SemaphoreType.DMA((count,))
            for count in (2, 2, 2, 2, chans - 1, chans - 1, 4 * bits, 4 * bits)
        ],
        compiler_params=pltpu.CompilerParams(collective_id=0, has_side_effects=True),
    )(*arrays)
    anywhere = pl.BlockSpec(memory_space=pl.ANY)
    placed = pl.pallas_call(
        functools.partial(place, len(outs)),
        out_shape=tuple(jax.ShapeDtypeStruct(out.shape, out.dtype) for out in outs),
        in_specs=[vmem] * len(outs),
        out_specs=(anywhere,) * len(outs),
        scratch_shapes=[pltpu.SemaphoreType.DMA((len(outs),))],
    )(*(pltpu.with_memory_space_constraint(out, pltpu.VMEM) for out in outs))
    return tuple(out.T for out in placed)


def solution(mesh):
    placed = (
        P("band", None),
        P(),
        P(None, "chan"),
        P(None, "chan"),
        P("band", None),
        P("band", "chan"),
        P("band", None, None),
        P("band"),
        P("band"),
    )
    return jax.shard_map(
        on_device,
        mesh=mesh,
        in_specs=placed,
        out_specs=(P("band", "chan"), P(None, "chan"), P(None, "chan"), P(None, "chan")),
        check_vma=False,
    )
```

```python
import functools
import math

import jax
import jax.numpy as jnp
from jax import lax
from jax.experimental import pallas as pl
from jax.experimental.pallas import tpu as pltpu
from jax.sharding import PartitionSpec as P

BF = jnp.bfloat16
F32 = jnp.float32
MESH = pl.DeviceIdType.MESH


def mm(a, b):
    return lax.dot_general(a, b, (((1,), (0,)), ((), ())), preferred_element_type=F32)


def mm_tn(a, b):
    return lax.dot_general(a, b, (((0,), (0,)), ((), ())), preferred_element_type=F32)


def mm_nt(a, b):
    return lax.dot_general(a, b, (((1,), (1,)), ((), ())), preferred_element_type=F32)


def eye(size):
    row = lax.broadcasted_iota(jnp.int32, (size, size), 0)
    col = lax.broadcasted_iota(jnp.int32, (size, size), 1)
    return jnp.where(row == col, 1.0, 0.0).astype(BF)


def sigmoid(v):
    return 0.5 + 0.5 * jnp.tanh(0.5 * v)


def flip(index, bit):
    step = 1 << bit
    return index + step - 2 * step * lax.rem(lax.div(index, step), 2)


def body(
    bands, chans, chunk,
    feat_in, embed_in, wsend_in, wrecv_in, nodes_in, cot_in, send_in, source_in, receiver_in,
    mesh_out, late_out, send_out, recv_out,
    feat, embed, wsend, wrecv, nodes, cot, send, source, receiver, loads,
    latent, back_weight, outgoing, outer, tables, acc, hot_recv, drawn_recv, slots_out, returned, back_out, back_in,
    xs1, xr1, snd1, rcv1, fin1, xs2, xr2, snd2, rcv2, fin2,
    row_send, row_recv, ret_send, ret_recv, back_send, back_recv, sum_send, sum_recv,
):
    band = lax.axis_index("band")
    chan = lax.axis_index("chan")
    bits = bands.bit_length() - 1
    width = wsend.shape[0]
    grid = feat.shape[1]
    mesh_count = nodes.shape[0]
    cap = outgoing.shape[0] // 2
    slots = grid + 2 * cap
    half = width // 2
    left = lax.rem(band + bands - 1, bands)
    right = lax.rem(band + 1, bands)
    partners = [flip(band, bit) for bit in range(bits)]
    others = [lax.rem(chan + step, chans) for step in range(1, chans)]

    barrier = pltpu.get_barrier_semaphore()
    for peer in [left, right] + partners[1:]:
        pl.semaphore_signal(barrier, inc=1, device_id=(peer, chan), device_id_type=MESH)
    for peer in others:
        pl.semaphore_signal(barrier, inc=1, device_id=(band, peer), device_id_type=MESH)

    pulls = {}
    for at, (name, src, dst) in enumerate(
        (
            ("feat", feat_in, feat), ("embed", embed_in, embed), ("send", send_in, send),
            ("wsend", wsend_in, wsend), ("nodes", nodes_in, nodes), ("wrecv", wrecv_in, wrecv),
            ("cot", cot_in, cot), ("source", source_in, source), ("receiver", receiver_in, receiver),
        )
    ):
        pulls[name] = pltpu.make_async_copy(src, dst, loads.at[at])
        pulls[name].start()

    def remote(src, dst, send_sem, recv_sem, to_band, to_chan):
        return pltpu.make_async_remote_copy(
            src_ref=src, dst_ref=dst, send_sem=send_sem, recv_sem=recv_sem,
            device_id=(to_band, to_chan), device_id_type=MESH,
        )

    pulls["send"].wait()
    picks = lax.broadcasted_iota(jnp.int32, (grid, 2 * cap), 0) == jnp.concatenate(
        [send[0, 0:1, :], send[0, 1:2, :]], axis=1
    )
    pick_rows = jnp.transpose(jnp.where(picks, 1.0, 0.0)).astype(BF)
    pulls["feat"].wait()
    pulls["embed"].wait()
    grid_pre = mm_tn(feat[...], embed[...])
    latent[...] = (grid_pre * sigmoid(grid_pre)).astype(BF)
    pulls["wsend"].wait()
    own = mm_nt(wsend[...], latent[...]).astype(BF)
    outgoing[...] = mm_nt(pick_rows, own).astype(BF)
    pl.semaphore_wait(barrier, 2 + (bits - 1) + (chans - 1))
    low, high = pl.ds(0, cap), pl.ds(cap, cap)
    rows = [
        remote(outgoing.at[low], outer.at[high], row_send.at[0], row_recv.at[0], left, chan),
        remote(outgoing.at[high], outer.at[low], row_send.at[1], row_recv.at[1], right, chan),
    ]
    for copy in rows:
        copy.start()

    turn = eye(width)
    for name in ("nodes", "wrecv", "cot", "source", "receiver"):
        pulls[name].wait()
    tables[:width, :grid] = own
    tables[:width, slots:] = mm_nt(wrecv[...], nodes[...]).astype(BF)
    tables[width:, slots:] = cot[...]
    acc[...] = jnp.zeros_like(acc)
    back_weight[...] = mm_nt(eye(wsend.shape[1]), wsend[...]).astype(BF)
    choose = lax.broadcasted_iota(jnp.int32, (width, embed.shape[1]), 1) == (
        lax.broadcasted_iota(jnp.int32, (width, embed.shape[1]), 0) + chan * width
    )
    mine = mm_nt(jnp.where(choose, 1.0, 0.0).astype(BF), embed[...]).astype(BF)
    pre_mine = mm(mine, feat[...])
    gate = sigmoid(pre_mine)
    slope_mine = gate * (1.0 + pre_mine * (1.0 - gate))

    def one_hot(index, count, step):
        at = index[pl.ds(pl.multiple_of(step * chunk, chunk), chunk)].reshape(1, chunk)
        hit = lax.broadcasted_iota(jnp.int32, (count, chunk), 0) == at
        return jnp.where(hit, 1.0, 0.0).astype(BF)

    def receivers(step, carry):
        hot = one_hot(receiver, mesh_count, step)
        hot_recv[step] = hot
        drawn_recv[step] = mm(tables[:, slots:], hot)
        return carry

    steps = source.shape[0] // chunk
    lax.fori_loop(0, steps, receivers, 0)
    for copy in rows:
        copy.wait()
    tables[:width, grid:slots] = mm_nt(turn, outer[...]).astype(BF)

    def edges(step, carry):
        hot = one_hot(source, slots, step)
        pre = mm(tables[:width, :slots], hot) + drawn_recv[step, :width, :]
        gate = sigmoid(pre)
        message = pre * gate
        grad = drawn_recv[step, width:, :] * (gate + message * (1.0 - gate))
        both = jnp.concatenate([message, grad], axis=0).astype(BF)
        acc[width:, :slots] += mm_nt(both[width:], hot)
        acc[:, slots:] += mm_nt(both, hot_recv[step])
        return carry

    lax.fori_loop(0, steps, edges, 0)

    slots_out[...] = mm_nt(eye(2 * cap), acc[width:, grid:slots].astype(BF)).astype(BF)
    backs = [
        remote(slots_out.at[low], returned.at[high], ret_send.at[0], ret_recv.at[0], left, chan),
        remote(slots_out.at[high], returned.at[low], ret_send.at[1], ret_recv.at[1], right, chan),
    ]
    for copy in backs:
        copy.start()
    latents = embed.shape[1]
    xs1[:, :latents] = mm(acc[width:, slots:].astype(BF), nodes[...]).astype(BF)
    mesh_out[...] = acc[:width, slots:].astype(BF)
    for copy in backs:
        copy.wait()
    ret_t = mm_nt(turn, returned[...]).astype(BF)
    total = (acc[width:, :grid].astype(BF).astype(F32) + mm(ret_t, pick_rows)).astype(BF)

    sums = []
    for at, peer in enumerate(others):
        block = back_weight[pl.ds(pl.multiple_of(peer * width, width), width), :]
        back_out[at] = mm(block, total).astype(BF)
        copy = remote(back_out.at[at], back_in.at[at], back_send.at[at], back_recv.at[at], band, peer)
        copy.start()
        sums.append(copy)
    grid_grad = mm(back_weight[pl.ds(pl.multiple_of(chan * width, width), width), :], total)
    xs1[:, latents:] = mm(total, latent[...]).astype(BF)

    my_half = pl.ds(pl.multiple_of(lax.rem(band, 2) * half, half), half)
    its_half = pl.ds(pl.multiple_of((1 - lax.rem(band, 2)) * half, half), half)

    def reduction(base, xs, xr, snd, rcv, fin):
        middle = xs.shape[1] // 2
        copy = remote(
            xs.at[its_half], xr, sum_send.at[base], sum_recv.at[base], partners[0], chan
        )
        copy.start()
        yield
        copy.wait()
        value = xs[my_half, :].astype(F32) + xr[...].astype(F32)
        for at in range(bits - 1):
            snd[at] = value.astype(BF)
            pair = []
            for side, bit in enumerate((1 + at, bits - 1 - at)):
                cut = pl.ds(side * middle, middle)
                sem = base + 1 + 2 * at + side
                pair.append(
                    remote(
                        snd.at[at, :, cut], rcv.at[at, :, cut],
                        sum_send.at[sem], sum_recv.at[sem], partners[bit], chan,
                    )
                )
            for copy in pair:
                copy.start()
            yield
            for copy in pair:
                copy.wait()
            value = snd[at].astype(F32) + rcv[at].astype(F32)
        fin[my_half, :] = value
        sem = base + 1 + 2 * (bits - 1)
        copy = remote(
            fin.at[my_half], fin.at[my_half], sum_send.at[sem], sum_recv.at[sem], partners[0], chan
        )
        copy.start()
        yield
        copy.wait()
        yield

    early = reduction(0, xs1, xr1, snd1, rcv1, fin1)
    late = reduction(2 * bits, xs2, xr2, snd2, rcv2, fin2)
    for _ in range(bits):
        next(early)
    for at, copy in enumerate(sums):
        copy.wait()
        grid_grad = grid_grad + back_in[at].astype(F32)
    pre_grad = (grid_grad * slope_mine).astype(BF)
    inputs = feat.shape[0]
    if inputs < xs2.shape[1]:
        xs2[...] = jnp.zeros_like(xs2)
    xs2[:, :inputs] = mm_nt(pre_grad, feat[...]).astype(BF)
    next(late)
    next(early)
    next(late)
    next(early)
    recv_out[...] = fin1[:, :latents]
    send_out[...] = fin1[:, latents:]
    for _ in range(bits):
        next(late)
    late_out[...] = fin2[:, :inputs]


def place(count, *refs):
    sems = refs[2 * count]
    copies = [
        pltpu.make_async_copy(refs[at], refs[count + at], sems.at[at]) for at in range(count)
    ]
    for copy in copies:
        copy.start()
    for copy in copies:
        copy.wait()


def on_device(
    grid_feat, w_embed, w_send, w_recv, mesh_nodes, mesh_cot, send_index, edge_source, edge_receiver
):
    bands = lax.axis_size("band")
    chans = lax.axis_size("chan")
    bits = bands.bit_length() - 1
    grid, inputs = grid_feat.shape
    latents, width = w_send.shape
    mesh_count = mesh_nodes.shape[0]
    cap = send_index.shape[2]
    slots = grid + 2 * cap
    half = width // 2
    chunk = math.gcd(edge_source.shape[0], 1024)
    wide1 = 2 * latents
    wide2 = -(-inputs // 256) * 256
    steps = max(bits - 1, 1)
    vmem = pl.BlockSpec(memory_space=pltpu.VMEM)
    arrays = (
        grid_feat.T, w_embed, w_send.T, w_recv.T, mesh_nodes, mesh_cot.T,
        send_index, edge_source, edge_receiver,
    )
    outs = pl.pallas_call(
        functools.partial(body, bands, chans, chunk),
        out_shape=(
            pltpu.VMEM((width, mesh_count), BF),
            pltpu.VMEM((width, inputs), F32),
            pltpu.VMEM((width, latents), F32),
            pltpu.VMEM((width, latents), F32),
        ),
        in_specs=[pl.BlockSpec(memory_space=pl.ANY)] * 9,
        out_specs=(vmem,) * 4,
        scratch_shapes=[
            pltpu.VMEM(array.shape, array.dtype) for array in arrays
        ]
        + [
            pltpu.SemaphoreType.DMA((9,)),
            pltpu.VMEM((grid, latents), BF),
            pltpu.VMEM((latents, width), BF),
            pltpu.VMEM((2 * cap, width), BF),
            pltpu.VMEM((2 * cap, width), BF),
            pltpu.VMEM((2 * width, slots + mesh_count), BF),
            pltpu.VMEM((2 * width, slots + mesh_count), F32),
            pltpu.VMEM((edge_source.shape[0] // chunk, mesh_count, chunk), BF),
            pltpu.VMEM((edge_source.shape[0] // chunk, 2 * width, chunk), F32),
            pltpu.VMEM((2 * cap, width), BF),
            pltpu.VMEM((2 * cap, width), BF),
            pltpu.VMEM((chans - 1, width, grid), BF),
            pltpu.VMEM((chans - 1, width, grid), BF),
        ]
        + [
            pltpu.VMEM(shape, kind)
            for wide in (wide1, wide2)
            for shape, kind in (
                ((width, wide), BF),
                ((half, wide), BF),
                ((steps, half, wide), BF),
                ((steps, half, wide), BF),
                ((width, wide), F32),
            )
        ]
        + [
            pltpu.SemaphoreType.DMA((count,))
            for count in (2, 2, 2, 2, chans - 1, chans - 1, 4 * bits, 4 * bits)
        ],
        compiler_params=pltpu.CompilerParams(collective_id=0, has_side_effects=True),
    )(*arrays)
    anywhere = pl.BlockSpec(memory_space=pl.ANY)
    placed = pl.pallas_call(
        functools.partial(place, len(outs)),
        out_shape=tuple(jax.ShapeDtypeStruct(out.shape, out.dtype) for out in outs),
        in_specs=[vmem] * len(outs),
        out_specs=(anywhere,) * len(outs),
        scratch_shapes=[pltpu.SemaphoreType.DMA((len(outs),))],
    )(*(pltpu.with_memory_space_constraint(out, pltpu.VMEM) for out in outs))
    return tuple(out.T for out in placed)


def solution(mesh):
    placed = (
        P("band", None),
        P(),
        P(None, "chan"),
        P(None, "chan"),
        P("band", None),
        P("band", "chan"),
        P("band", None, None),
        P("band"),
        P("band"),
    )
    return jax.shard_map(
        on_device,
        mesh=mesh,
        in_specs=placed,
        out_specs=(P("band", "chan"), P(None, "chan"), P(None, "chan"), P(None, "chan")),
        check_vma=False,
    )
```
